32 devices in a mesh: seq: 8 (over z, core), head: 4 (over y, x).
Axes of the slice: x: 2, y: 2, z: 4, core: 2. Of those that a mesh axis runs over, the one named last changes fastest.
Arguments:
- tokens: bfloat16 [1024, 4096], P('seq', 'head'), may hold values from -6 to 6
- w_query: bfloat16 [4096, 4096], P(None, 'head'), may hold values from -0.09375 to 0.09375
- w_key: bfloat16 [4096, 4096], P(None, 'head'), may hold values from -0.09375 to 0.09375
- w_value: bfloat16 [4096, 4096], P(None, 'head'), may hold values from -0.09375 to 0.09375
- upstream: bfloat16 [1024, 4096], P('seq', 'head'), may hold values from -6 to 6
- log_decay: float32 [1024, 32], P('seq', 'head'), may hold values from -1 to 0, as said below
- segment: int32 [1024], replicated, may hold values from 0 to 7, never falling along the last dimension, each value on 1 to 256 neighbouring positions
Outputs:
- grad_query: bfloat16 [4096, 4096], P('seq', 'head')
- grad_key: bfloat16 [4096, 4096], P('seq', 'head')
- grad_value: bfloat16 [4096, 4096], P('seq', 'head')
The draws below stay inside these ranges and needn't reach their ends.
Inputs may be any that keep to these rules, and one draw needn't show every extreme that they name: log_decay is negative. `segment`: document ids never fall along the tokens; each document holds 1 to 256 tokens.
All inputs are finite; a program needn't handle non-finite values.
Results may differ from the reference program's by a relative error of at most 0.02.
Values may be sent and summed in bfloat16 or wider, within the bound.
A program may use at most 64 MiB of HBM per device.

```python
import math
import jax
import jax.numpy as jnp
import numpy as np
from jax import lax

D = 4096
HEAD_COUNT = 32
HEAD = 128
TOK_DEV = 128
DOCS = 8
TOKEN_COUNT = 1024
N_SEQ = 8


def draw_log_decay(key, part):
    document_lanes = jax.random.split(key, 6)
    fast_share = 0.5
    fast = jax.random.uniform(document_lanes[0], (HEAD_COUNT,)) < fast_share
    slow_rate = jax.random.uniform(document_lanes[1], (HEAD_COUNT,), minval=0.1, maxval=0.4) * math.log(10.0) / TOKEN_COUNT
    fast_rate = 1.0 / jax.random.uniform(document_lanes[2], (HEAD_COUNT,), minval=30.0, maxval=50.0)
    decay_rate = jnp.where(fast, fast_rate, slow_rate)
    coarse_estimate = jnp.exp(jax.random.uniform(document_lanes[3], (TOKEN_COUNT, HEAD_COUNT), minval=-math.log(2.0), maxval=math.log(2.0)))
    decay_jump = jax.random.uniform(document_lanes[4], (TOKEN_COUNT, HEAD_COUNT)) < 2.0 / TOKEN_COUNT
    feature_depth = jax.random.uniform(document_lanes[5], (TOKEN_COUNT, HEAD_COUNT), minval=0.22, maxval=0.69)
    return (-(decay_rate[None, :] * coarse_estimate) - jnp.where(decay_jump, feature_depth, 0.0)).astype(jnp.float32)


def strengthened(values, stream_key, source, target, parts, factor):
    owner, partner = [(jnp.arange(values.shape[dim]) // (values.shape[dim] // parts)).reshape([-1 if axis == dim else 1 for axis in range(values.ndim)]) for dim in (source, target)]
    chosen = jax.random.permutation(stream_key, parts)[partner]
    strong = (owner == chosen) | (owner == (partner + parts // 2) % parts)
    return jnp.where(strong, factor * values, values)


def steps_of(key, extent, cuts, smallest, high):
    def one(axis_at, blocks):
        draws = jax.random.uniform(jax.random.fold_in(jax.random.fold_in(key, 6), axis_at), (blocks,), jnp.float32, smallest / len(cuts), high / len(cuts))
        return jnp.repeat(jnp.exp(draws), extent[axis_at] // blocks).reshape((-1,) + (1,) * (len(extent) - axis_at - 1))

    gain = one(*cuts[0])
    for cut in cuts[1:]:
        gain = gain * one(*cut)
    return gain


def profile(count, total, limit, lean):
    weights = [(1 << 20) // math.isqrt(rank ** lean) + 1 for rank in range(2, count + 1)]
    surplus, holding = total - limit - (count - 1), [1] * (count - 1)
    while surplus > 0:
        movable = [i for i in range(count - 1) if holding[i] < limit]
        pool, remaining = sum([weights[i] for i in movable]), surplus
        for i in movable:
            more = min(limit - holding[i], max(1, remaining * weights[i] // pool), surplus)
            holding[i] = holding[i] + more
            surplus = surplus - more
    return np.array([limit] + holding)


def uneven(rng, number_of, total, reach, lean):
    if number_of == 2:
        one = jax.random.randint(rng, (), max(1, total - reach), min(reach, total - 1) + 1)
        return jnp.stack([one, total - one])
    tallies = jnp.asarray(profile(number_of, total, reach, lean), jnp.int32)
    pairs = (number_of - 1) // 2
    donor, taker = tallies[1:1 + 2 * pairs:2], tallies[2:2 + 2 * pairs:2]
    room = jnp.minimum(donor - 1, reach - taker)
    moved = jax.random.randint(jax.random.fold_in(rng, 1), (pairs,), 0, 1 << 20) % (room + 1)
    tallies = tallies.at[1:1 + 2 * pairs:2].set(donor - moved).at[2:2 + 2 * pairs:2].set(taker + moved)
    return tallies[jax.random.permutation(jax.random.fold_in(rng, 2), number_of)]


def scatter_about(own_key, dims, scale, reach, cuts=(), kind=jnp.bfloat16):
    result = scale * jax.random.normal(own_key, dims, jnp.float32)
    if cuts:
        result = result * steps_of(own_key, dims, cuts, -0.22, 0.18)
    return jnp.clip(result, -reach, reach).astype(kind)


def heavy_noise(rng, extent, scale, reach, shards, heavy, held_as=jnp.bfloat16):
    values = scale * jax.random.normal(rng, extent, jnp.float32)
    if shards:
        values = values * steps_of(rng, extent, shards, -0.22, 0.18)
    return jnp.clip(strengthened(values, jax.random.fold_in(rng, 3), *heavy), -reach, reach).astype(held_as)


def setup_inputs(seed: int = 0) -> dict:
    key_list = jax.random.split(jax.random.key(seed), 8)
    return {
        "tokens": heavy_noise(key_list[0], (TOKEN_COUNT, D), 1.0, 6.0, ((0, 8), (1, 4)), (0, 1, 8, 2.0)),
        "w_query": scatter_about(key_list[1], (D, HEAD_COUNT * HEAD), D ** -0.5, 0.09375, ((1, 4),)),
        "w_key": scatter_about(key_list[2], (D, HEAD_COUNT * HEAD), D ** -0.5, 0.09375, ((1, 4),)),
        "w_value": scatter_about(key_list[3], (D, HEAD_COUNT * HEAD), D ** -0.5, 0.09375, ((1, 4),)),
        "upstream": scatter_about(key_list[4], (TOKEN_COUNT, HEAD_COUNT * HEAD), 1.0, 6.0, ((0, 8), (1, 4))),
        "log_decay": draw_log_decay(jax.random.fold_in(key_list[7], 71), 0),
        "segment": jnp.searchsorted(jnp.cumsum(uneven(key_list[6], DOCS, TOKEN_COUNT, TOKEN_COUNT // 4, 0)), jnp.arange(TOKEN_COUNT), side="right").astype(jnp.int32),
    }


def rounded(array):
    return lax.optimization_barrier(array.astype(jnp.bfloat16)).astype(jnp.float32)

def block_factors(log_rates, segs, previous):
    log_sum = jnp.cumsum(log_rates, axis=0)
    last_sum = log_sum[-1]
    last_seg = segs[-1]
    state_entering = jnp.where((segs == previous)[:, None], jnp.exp(log_sum), 0.0)
    state_leaving = jnp.where((segs == last_seg)[:, None], jnp.exp(last_sum[None, :] - log_sum), 0.0)
    carry_decay = jnp.where(last_seg == previous, jnp.exp(last_sum), 0.0)
    places = jnp.arange(segs.shape[0], dtype=jnp.int32)
    same = (segs[:, None] == segs[None, :]) & (places[:, None] >= places[None, :])
    spread = log_sum.T[:, :, None] - log_sum.T[:, None, :]
    decay_mat = jnp.where(same[None], HEAD ** (-0.5) * jnp.exp(jnp.where(same[None], spread, 0.0)), 0.0)
    return (state_entering, state_leaving, carry_decay, decay_mat)

def summaries(block):
    query, key_rows, value_rows, upstream, log_rates, segs, previous = block
    state_entering, state_leaving, carry_decay, decay_mat = block_factors(log_rates, segs, previous)
    scale = HEAD ** (-0.5)
    weighted_keys = rounded(scale * state_leaving[:, :, None] * key_rows.astype(jnp.float32))
    segment_state = jnp.einsum('bdw,bdq->dwq', weighted_keys, value_rows.astype(jnp.float32), precision=lax.Precision.HIGHEST)
    weighted_queries = rounded(scale * state_entering[:, :, None] * query.astype(jnp.float32))
    following_state = jnp.einsum('bdw,bdq->dwq', weighted_queries, upstream.astype(jnp.float32), precision=lax.Precision.HIGHEST)
    return (carry_decay, segment_state, following_state)

def block_grads(block):
    query, key_rows, value_rows, upstream, log_rates, segs, previous, arriving_state, backward_state = block
    state_entering, state_leaving, carry_decay, decay_mat = block_factors(log_rates, segs, previous)
    query_rows_float = query.astype(jnp.float32)
    key_rows_float = key_rows.astype(jnp.float32)
    value_rows_float = value_rows.astype(jnp.float32)
    upstream_float = upstream.astype(jnp.float32)
    upper_limit = lax.Precision.HIGHEST
    attention_query_key = rounded(decay_mat * jnp.einsum('thd,shd->hts', query_rows_float, key_rows_float, precision=upper_limit))
    attention_upstream = rounded(decay_mat * jnp.einsum('thd,shd->hts', upstream_float, value_rows_float, precision=upper_limit))
    query_gradient = jnp.einsum('wcz,zwm->cwm', attention_upstream, key_rows_float, precision=upper_limit) + state_entering[:, :, None] * jnp.einsum('pzo,zao->pza', upstream_float, arriving_state, precision=upper_limit)
    key_gradient = jnp.einsum('voi,ovw->ivw', attention_upstream, query_rows_float, precision=upper_limit) + state_leaving[:, :, None] * jnp.einsum('ixz,xqz->ixq', value_rows_float, backward_state, precision=upper_limit)
    value_gradient = jnp.einsum('voi,ovw->ivw', attention_query_key, upstream_float, precision=upper_limit) + state_leaving[:, :, None] * jnp.einsum('dqg,qgf->dqf', key_rows_float, backward_state, precision=upper_limit)
    return (query_gradient.astype(jnp.bfloat16), key_gradient.astype(jnp.bfloat16), value_gradient.astype(jnp.bfloat16))

def reference(tokens, w_query, w_key, w_value, upstream, log_decay, segment):
    blocks = N_SEQ
    width = HEAD_COUNT * HEAD

    def project(weight):
        product = jnp.dot(tokens, weight, preferred_element_type=jnp.float32).astype(jnp.bfloat16)
        return product.reshape(blocks, TOK_DEV, HEAD_COUNT, HEAD)
    query = project(w_query)
    key_rows = project(w_key)
    value_rows = project(w_value)
    grads_up = upstream.reshape(blocks, TOK_DEV, HEAD_COUNT, HEAD)
    rates = log_decay.reshape(blocks, TOK_DEV, HEAD_COUNT)
    segs = segment.reshape(blocks, TOK_DEV)
    previous = jnp.concatenate([jnp.full((1,), -1, jnp.int32), segs[:-1, -1]])
    decays, local_states, later_states = lax.map(summaries, (query, key_rows, value_rows, grads_up, rates, segs, previous))

    def forward(state, item):
        decay, segment_state = item
        return (decay[:, None, None] * state + segment_state, state)
    zeros = jnp.zeros((HEAD_COUNT, HEAD, HEAD), jnp.float32)
    _, arriving_state = lax.scan(forward, zeros, (decays, local_states))
    _, backward_state = lax.scan(forward, zeros, (decays, later_states), reverse=True)
    query_gradient, key_gradient, value_gradient = lax.map(block_grads, (query, key_rows, value_rows, grads_up, rates, segs, previous, arriving_state, backward_state))

    def weight_grad(grads):
        flat = grads.reshape(TOKEN_COUNT, width)
        return jnp.dot(tokens.T, flat, preferred_element_type=jnp.float32).astype(jnp.bfloat16)
    return (weight_grad(query_gradient), weight_grad(key_gradient), weight_grad(value_gradient))
```

```python
import functools

import jax
import jax.numpy as jnp
from jax import lax
from jax.experimental import pallas as pl
from jax.experimental.pallas import tpu as pltpu
from jax.sharding import PartitionSpec as P

HEAD = 128
SCALE = HEAD ** (-0.5)
MESH = pl.DeviceIdType.MESH
VMEM_BYTES = 56 * 1024 * 1024


def dot(a, b, contract=((1,), (0,))):
    return lax.dot_general(a, b, (contract, ((), ())), preferred_element_type=jnp.float32)


def half(x):
    return x.astype(jnp.bfloat16)


def aligned(index, size):
    return pl.ds(pl.multiple_of(index * size, size), size)


def kernel(nz, nh, heads, reach, tok_ref, up_ref, dec_ref, seg_ref, wq_ref, wk_ref, wv_ref, oq_ref, ok_ref, ov_ref, T, U, L, W, q_s, k_s, v_s, acc, D, IN, OUT, CR, LT, R, A, TT, G, zs, zr, uas, uar, ubs, ubr, xs, xr, ds, dr, ps, pr, qs, qr, es, er, ls, lr, own, wsem):
    s, h = lax.axis_index("seq"), lax.axis_index("head")
    z, c = s // 2, s % 2
    nb = 2 * nz
    rows, feat = tok_ref.shape
    width = heads * HEAD
    mate = z * 2 + 1 - c
    relay = nh == 4
    parts = 2 if relay else 1
    piece = feat // parts
    span = (reach + 1) // 2
    lag = max(span, nz - 3)

    def flip(a):
        hi, lo = h // 2, h % 2
        hi = 1 - hi if a // 2 else hi
        lo = 1 - lo if a % 2 else lo
        return hi * 2 + lo

    others = [flip(a) for a in (1, 2, 3)] if relay else [lax.rem(h + a, nh) for a in range(1, nh)]
    sides = 2 if relay else nh - 1
    barrier = pltpu.get_barrier_semaphore()
    targets = [(lax.rem(s + k, nb), h) for k in range(1, nb)] + [(s, o) for o in others]
    for target in targets:
        pl.semaphore_signal(barrier, inc=1, device_id=target, device_id_type=MESH)

    lower = z * 2 < nz
    near = jnp.where(lower, z, nz - 1 - z)

    def turned(pos):
        return jnp.where(lower, pos, nz - 1 - pos)

    def order(p):
        step = (p + 1) // 2
        pos = jnp.where(p > 2 * near, p, jnp.where(p % 2 == 1, near - step, near + step))
        return turned(pos)

    def place(zz, cc, hh, lo=0, size=feat):
        return T.at[aligned(zz * 2 + cc, rows), pl.ds(pl.multiple_of(hh * feat + lo, 128), size)]

    def uplace(zz, cc):
        return U.at[aligned(zz * 2 + cc, rows), :]

    def remote(src, dst, ss, rs, target):
        return pltpu.make_async_remote_copy(src_ref=src, dst_ref=dst, send_sem=ss, recv_sem=rs, device_id=target, device_id_type=MESH)

    my_up = up_ref.at[:, aligned(c, width)]
    their_up = up_ref.at[:, aligned(1 - c, width)]
    stays = [
        pltpu.make_async_copy(tok_ref, place(z, c, h), own.at[0]),
        pltpu.make_async_copy(my_up, uplace(z, c), own.at[1]),
        pltpu.make_async_copy(dec_ref, L.at[s], own.at[2]),
    ]

    def weight(hh):
        at = aligned(hh, feat)
        return [
            pltpu.make_async_copy(w_ref.at[at, aligned(c, width)], W.at[n, at, :], wsem.at[hh, n])
            for n, w_ref in enumerate((wq_ref, wk_ref, wv_ref))
        ]

    everyone = [h] + others
    for copy in stays:
        copy.start()
    for hh in everyone:
        for copy in weight(hh):
            copy.start()

    def z_copy(src, zz, up):
        to = (z + 1 if up else z - 1) * 2 + c
        return remote(src, place(zz, c, h), zs.at[up, zz], zr.at[zz], (to, h))

    def ua_copy(src, zz, up):
        to = (z + 1 if up else z - 1) * 2 + c
        return remote(src, uplace(zz, c), uas.at[up, zz], uar.at[zz], (to, h))

    def ub_copy(zz, up):
        to = (z + 1 if up else z - 1) * 2 + c
        return remote(uplace(zz, 1 - c), uplace(zz, 1 - c), ubs.at[up, zz], ubr.at[zz], (to, h))

    def side_copy(src, zz, j, n):
        lo = n * piece
        return remote(src.at[:, pl.ds(lo, piece)], place(zz, c, h, lo, piece), xs.at[j, n, zz], xr.at[j, n, zz], (s, others[j]))

    def side_arrival(zz, j, n):
        here = place(zz, c, others[j], n * piece, piece)
        return remote(here, here, xs.at[j, n, zz], xr.at[j if relay else nh - 2 - j, n, zz], (mate, h))

    def diag_copy(zz, j):
        part = place(zz, c, others[j], j * piece, piece)
        return remote(part, part, ds.at[j, zz], dr.at[j, zz], (s, others[1 - j]))

    def diag_arrival(zz, j):
        part = place(zz, c, others[2], j * piece, piece)
        return remote(part, part, ds.at[j, zz], dr.at[j, zz], (mate, h))

    def mate_copy(src, zz, hh):
        return remote(src, place(zz, c, hh), ps.at[zz, hh], pr.at[zz, hh], (mate, h))

    def mate_arrival(zz, hh):
        there = place(zz, 1 - c, hh)
        return remote(there, there, ps.at[zz, hh], pr.at[zz, hh], (mate, h))

    def swap(b):
        return remote(A.at[0, aligned(b, rows)], A.at[1, aligned(b, rows)], es.at[b], er.at[b], (mate, h))

    mate_up = remote(their_up, uplace(z, c), qs.at[0], qr.at[0], (mate, h))
    small = [remote(dec_ref, L.at[s], ls.at[k], lr.at[k], (lax.rem(s + k, nb), h)) for k in range(1, nb)]

    def spread(src, zz):
        for j in range(sides):
            side_copy(src, zz, j, j if relay else 0).start()
        if relay:
            for j in range(sides):
                side_copy(src, zz, j, 1 - j).start()
        mate_copy(src, zz, h).start()

    goes_up, goes_down = z + 1 < nz, z >= 1

    def along(zz, what):
        @pl.when((zz <= z) & goes_up)
        def _():
            what(1)

        @pl.when((zz >= z) & goes_down)
        def _():
            what(0)

    def each(k, what):
        @pl.when(z - k >= 0)
        def _():
            what(z - k)

        @pl.when(z + k < nz)
        def _():
            what(z + k)

    def passed(zz):
        return ((zz < z) & goes_up) | ((zz > z) & goes_down)

    def take_z(k):
        def one(zz):
            here = place(zz, c, h)
            z_copy(here, zz, 0).wait_recv()

            def forward(up):
                z_copy(here, zz, up).start()

                @pl.when(k == 1)
                def _():
                    ub_copy(z, up).start()

            along(zz, forward)

        each(k, one)

    def wait_u(zz):
        ua_copy(uplace(zz, c), zz, 0).wait_recv()
        ub_copy(zz, 0).wait_recv()

    def pass_u(zz):
        @pl.when(passed(zz))
        def _():
            wait_u(zz)

            def forward(up):
                ua_copy(uplace(zz, c), zz, up).start()
                ub_copy(zz, up).start()

            along(zz, forward)

    pl.semaphore_wait(barrier, len(targets))
    for copy in small:
        copy.start()
    along(z, lambda up: z_copy(tok_ref, z, up).start())
    spread(tok_ref, z)
    mate_up.start()
    along(z, lambda up: ua_copy(my_up, z, up).start())

    i = lax.broadcasted_iota(jnp.int32, (rows, rows), 0)
    j = lax.broadcasted_iota(jnp.int32, (rows, rows), 1)

    def wide(row):
        return jnp.broadcast_to(row, (rows, rows))

    zero = jnp.zeros((HEAD, HEAD), jnp.float32)
    for a in range(heads):
        for n in range(reach):
            for at in (n, nb + reach + n):
                LT[a, at] = zero
                R[a, at] = zero
                CR[a, at] = zero[:8]

    def clear(n, _):
        G[:, aligned(n, 8), :] = jnp.zeros((2, 8, G.shape[2]), jnp.float32)
        return 0

    lax.fori_loop(0, G.shape[1] // 8, clear, 0)
    for copy in stays:
        copy.wait()
    there = uplace(z, 1 - c)
    remote(there, there, qs.at[0], qr.at[0], (mate, h)).wait_recv()

    @pl.when(goes_up & (z == 0))
    def _():
        ub_copy(z, 1).start()

    @pl.when(goes_down & (z == nz - 1))
    def _():
        ub_copy(z, 0).start()

    for k in range(1, nb):
        there = L.at[lax.rem(s + nb - k, nb)]
        remote(there, there, ls.at[k], lr.at[k], (mate, h)).wait_recv()
    triangle = jnp.where(i <= j, 1.0, 0.0).astype(jnp.float32)
    L[...] = lax.dot_general(
        L[...].reshape(nb * L.shape[1], rows), triangle, (((1,), (0,)), ((), ())), precision=lax.Precision.HIGHEST, preferred_element_type=jnp.float32
    ).reshape(L.shape)

    def tables(b, _):
        segs = wide(seg_ref[pl.ds(b, 1), :].astype(jnp.float32))
        ahead = seg_ref[pl.ds(jnp.maximum(b - 1, 0), 1), rows - 1 :].astype(jnp.float32)
        before = wide(jnp.where(b == 0, -1.0, ahead))
        segs_down = segs.T
        last_seg = wide(segs[:1, rows - 1 :])
        same = (segs == segs_down) & (i >= j)
        for a in range(heads):
            ahead_sum = wide(L[b, pl.ds(c * heads + a, 1), :])
            down = ahead_sum.T
            last = wide(ahead_sum[:1, rows - 1 :])
            D[a, b] = jnp.where(same, SCALE * jnp.exp(jnp.where(same, down - ahead_sum, 0.0)), 0.0)
            IN[a, b] = jnp.where(segs_down == before, jnp.exp(down), 0.0)
            OUT[a, b] = jnp.where(segs_down == last_seg, jnp.exp(last - down), 0.0)
            CR[a, b + reach] = jnp.where(last_seg == before, jnp.exp(last), 0.0)[:8]
        return 0

    lax.fori_loop(0, nb, tables, 0)

    def pair(zz):
        return aligned(zz, 2 * rows)

    def project(zz, hh, first, done):
        mate_arrival(zz, hh).wait_recv()
        x = T[pair(zz), aligned(hh, feat)]
        for n, out in enumerate((q_s, k_s, v_s)):
            new = dot(x, W[n, aligned(hh, feat), :])
            cols = slice(n * width, (n + 1) * width)
            if not first:
                new = acc[:, cols] + new
            if done:
                out[pair(zz), :] = half(new)
            else:
                acc[:, cols] = new

    def cols(a):
        return slice(a * HEAD, (a + 1) * HEAD)

    def states(zz):
        def block(n, _):
            b = zz * 2 + n
            at = aligned(b, rows)
            for a in range(heads):
                weighted_k = half(OUT[a, b] * k_s[at, cols(a)].astype(jnp.float32))
                weighted_q = half(IN[a, b] * q_s[at, cols(a)].astype(jnp.float32))
                LT[a, b + reach] = dot(v_s[at, cols(a)], weighted_k, ((0,), (0,)))
                R[a, b + reach] = dot(weighted_q, U[at, cols(a)], ((0,), (0,)))
            return 0

        lax.fori_loop(0, 2, block, 0)

    def attend(zz):
        def block(n, _):
            b = zz * 2 + n
            at = aligned(b, rows)
            for a in range(heads):
                q, k, v, u = q_s[at, cols(a)], k_s[at, cols(a)], v_s[at, cols(a)], U[at, cols(a)]
                coming, back = LT[a, b], R[a, b + 2 * reach]
                for m in range(reach - 1, 0, -1):
                    coming = wide(CR[a, b + reach - m, :1]) * coming + LT[a, b + reach - m]
                    back = wide(CR[a, b + reach + m, :1]) * back + R[a, b + reach + m]
                coming, back = half(SCALE * coming), half(SCALE * back)
                decay, inflow, outflow = D[a, b], IN[a, b], OUT[a, b]
                attn_qk = half(decay * dot(q, k, ((1,), (1,))))
                attn_up = half(decay * dot(u, v, ((1,), (1,))))
                in_u = half(inflow * u.astype(jnp.float32))
                out_v = half(outflow * v.astype(jnp.float32))
                out_k = half(outflow * k.astype(jnp.float32))
                gq = dot(attn_up, k) + dot(in_u, coming)
                gk = dot(attn_up, q, ((0,), (0,))) + dot(out_v, back, ((1,), (1,)))
                gv = dot(attn_qk, u, ((0,), (0,))) + dot(out_k, back)
                for g, value in enumerate((gq, gk, gv)):
                    A[0, at, g * width + a * HEAD : g * width + (a + 1) * HEAD] = half(value)
            return 0

        lax.fori_loop(0, 2, block, 0)
        swap(zz * 2).start()
        swap(zz * 2 + 1).start()

    depth_rows = TT.shape[0]

    def turn(zz):
        TT[:, pair(zz)] = T[pair(zz), aligned(s, depth_rows)].T

    def gather(zz):
        swap(zz * 2).wait_recv()
        swap(zz * 2 + 1).wait_recv()
        for slot in range(2):
            for g in range(3):
                at = slice(g * width, (g + 1) * width)
                G[slot, :, at] += dot(TT[:, pair(zz)], A[slot, pair(zz), at])

    def step(p, _):
        zz = order(p)
        live = p < nz

        @pl.when(live)
        def _():
            for n in range(sides):
                side_arrival(zz, n, n if relay else 0).wait_recv()
                if relay:
                    diag_copy(zz, n).start()
                else:
                    mate_copy(place(zz, c, others[n]), zz, others[n]).start()

        @pl.when(p == 2)
        def _():
            each(1, pass_u)

        @pl.when((p >= 1) & (p <= nz))
        def _():
            old = order(p - 1)
            if relay:
                project(old, others[2], False, True)

            @pl.when((old != z) & jnp.logical_not(passed(old)))
            def _():
                wait_u(old)

            states(old)
            turn(old)

        @pl.when(live)
        def _():
            @pl.when(p == 0)
            def _():
                for copy in weight(h):
                    copy.wait()

            project(zz, h, True, False)

        @pl.when(p + 1 < nz)
        def _():
            take_z(p + 1)
            later = order(p + 1)
            spread(place(later, c, h), later)

        @pl.when((p >= 2) & (p < nz))
        def _():
            each(p, pass_u)

        if relay:
            @pl.when(live)
            def _():
                for n in range(sides):
                    side_arrival(zz, n, 1 - n).wait_recv()
                    mate_copy(place(zz, c, others[n]), zz, others[n]).start()

        @pl.when(p >= lag + 1)
        def _():
            attend(turned(p - lag - 1))

        @pl.when(live)
        def _():
            if relay:
                far = others[2]
                for n in range(2):
                    diag_arrival(zz, n).wait_recv()
                mate_copy(place(zz, c, far), zz, far).start()

            @pl.when(p == 0)
            def _():
                for hh in others:
                    for copy in weight(hh):
                        copy.wait()

            for n in range(sides):
                project(zz, others[n], False, (not relay) and n == sides - 1)

            @pl.when(p >= lag + 1)
            def _():
                gather(turned(p - lag - 1))

        return 0

    lax.fori_loop(0, nz + lag + 1, step, 0)
    lax.fori_loop(nz - lag - 1 if nz > lag else 0, nz - 1, lambda a, _: (gather(turned(a)), 0)[1], 0)

    final = turned(nz - 1)
    for slot in range(2):
        if slot == 1:
            swap(final * 2).wait_recv()
            swap(final * 2 + 1).wait_recv()
        put = aligned(c if slot == 0 else 1 - c, width)
        for g, out in enumerate((oq_ref, ok_ref, ov_ref)):
            at = slice(g * width, (g + 1) * width)
            out[:, put] = half(G[slot, :, at] + dot(TT[:, pair(final)], A[slot, pair(final), at]))

    def drain(zz, _):
        here = place(zz, c, h)

        def sent(up):
            z_copy(here, zz, up).wait_send()
            ua_copy(uplace(zz, c), zz, up).wait_send()
            ub_copy(zz, up).wait_send()

        along(zz, sent)
        for n in range(sides):
            for m in range(parts):
                side_copy(here, zz, n, m).wait_send()
        if relay:
            for n in range(2):
                diag_copy(zz, n).wait_send()
        for hh in everyone:
            mate_copy(place(zz, c, hh), zz, hh).wait_send()
        swap(zz * 2).wait_send()
        swap(zz * 2 + 1).wait_send()
        return 0

    lax.fori_loop(0, nz, drain, 0)
    mate_up.wait_send()
    for copy in small:
        copy.wait_send()


def local(n_seq, nh, tokens, w_query, w_key, w_value, upstream, log_decay, segment):
    nz = n_seq // 2
    rows, feat = tokens.shape
    total, depth = rows * n_seq, feat * nh
    heads = w_query.shape[1] // HEAD // 2
    width = heads * HEAD
    reach = total // 4 // rows
    parts = 2 if nh == 4 else 1
    decay = jnp.zeros((max(8, 2 * heads), rows), jnp.float32).at[: 2 * heads].set(log_decay.T)
    seg = segment.reshape(n_seq, rows)
    kind = tokens.dtype
    dma = pltpu.SemaphoreType.DMA
    vmem = pl.BlockSpec(memory_space=pltpu.VMEM)
    hbm = pl.BlockSpec(memory_space=pl.ANY)
    f32 = jnp.float32
    square = (HEAD, HEAD)
    padded = n_seq + 2 * reach
    out_rows = depth // n_seq
    return tuple(pl.pallas_call(
        functools.partial(kernel, nz, nh, heads, reach),
        out_shape=[pltpu.VMEM((out_rows, 2 * width), kind)] * 3,
        in_specs=[vmem] * 4 + [hbm] * 3,
        out_specs=[vmem] * 3,
        scratch_shapes=[
            pltpu.VMEM((total, depth), kind),
            pltpu.VMEM((total, width), kind),
            pltpu.VMEM((n_seq,) + decay.shape, f32),
            pltpu.VMEM((3, depth, width), kind),
        ]
        + [pltpu.VMEM((total, width), kind)] * 3
        + [pltpu.VMEM((2 * rows, 3 * width), f32)]
        + [pltpu.VMEM((heads, n_seq) + square, f32)] * 3
        + [pltpu.VMEM((heads, padded, 8, HEAD), f32)]
        + [pltpu.VMEM((heads, padded) + square, f32)] * 2
        + [
            pltpu.VMEM((2, total, 3 * width), kind),
            pltpu.VMEM((out_rows, total), kind),
            pltpu.VMEM((2, out_rows, 3 * width), f32),
        ]
        + [dma((2, nz)), dma((nz,))] * 3
        + [dma((nh - 1, parts, nz))] * 2
        + [dma((2, nz))] * 2
        + [dma((nz, nh))] * 2
        + [dma((1,))] * 2
        + [dma((n_seq,))] * 4
        + [dma((3,)), dma((nh, 3))],
        compiler_params=pltpu.CompilerParams(collective_id=0, has_side_effects=True, vmem_limit_bytes=VMEM_BYTES),
    )(tokens, upstream, decay, seg, w_query, w_key, w_value))


def solution(mesh):
    placed = (P("seq", "head"), P(None, "head"), P(None, "head"), P(None, "head"), P("seq", "head"), P("seq", "head"), P())
    return jax.shard_map(
        functools.partial(local, mesh.shape["seq"], mesh.shape["head"]),
        mesh=mesh,
        in_specs=placed,
        out_specs=(P("seq", "head"),) * 3,
        check_vma=False,
    )
```

```python
import functools

import jax
import jax.numpy as jnp
from jax import lax
from jax.experimental import pallas as pl
from jax.experimental.pallas import tpu as pltpu
from jax.sharding import PartitionSpec as P

HEAD = 128
SCALE = HEAD ** (-0.5)
MESH = pl.DeviceIdType.MESH
VMEM_BYTES = 57 * 1024 * 1024


def dot(a, b, contract=((1,), (0,))):
    return lax.dot_general(a, b, (contract, ((), ())), preferred_element_type=jnp.float32)


def half(x):
    return x.astype(jnp.bfloat16)


def whole(x):
    return x.astype(jnp.float32)


def aligned(index, size):
    return pl.ds(pl.multiple_of(index * size, size), size)


def kernel(nz, nh, heads, reach, tok_ref, up_ref, dec_ref, seg_in, wq_ref, wk_ref, wv_ref, oq_ref, ok_ref, ov_ref, T, U, L, seg_ref, W, q_s, k_s, v_s, acc, D, IN, OUT, CR, LT, R, A, B, TT, G, zs, zr, uas, uar, ubs, ubr, xs, xr, ds, dr, ps, pr, qs, qr, es, er, es2, er2, ls, lr, own, wsem):
    s, h = lax.axis_index("seq"), lax.axis_index("head")
    z, c = s // 2, s % 2
    nb = 2 * nz
    rows, feat = tok_ref.shape
    width = heads * HEAD
    mate = z * 2 + 1 - c
    relay = nh == 4
    parts = 2 if relay else 1
    piece = feat // parts
    span = (reach + 1) // 2
    lag = max(span, nz - 3)
    slots = B.shape[0] // (2 * rows)

    def flip(a):
        hi, lo = h // 2, h % 2
        hi = 1 - hi if a // 2 else hi
        lo = 1 - lo if a % 2 else lo
        return hi * 2 + lo

    others = [flip(a) for a in (1, 2, 3)] if relay else [lax.rem(h + a, nh) for a in range(1, nh)]
    sides = 2 if relay else nh - 1
    barrier = pltpu.get_barrier_semaphore()
    goes_up, goes_down = z + 1 < nz, z >= 1
    for target in [(mate, h)] + [(s, o) for o in others]:
        pl.semaphore_signal(barrier, inc=1, device_id=target, device_id_type=MESH)

    @pl.when(goes_up)
    def _():
        pl.semaphore_signal(barrier, inc=1, device_id=(s + 2, h), device_id_type=MESH)

    @pl.when(goes_down)
    def _():
        pl.semaphore_signal(barrier, inc=1, device_id=(s - 2, h), device_id_type=MESH)

    lower = z * 2 < nz
    near = jnp.where(lower, z, nz - 1 - z)

    def turned(pos):
        return jnp.where(lower, pos, nz - 1 - pos)

    def order(p):
        step = (p + 1) // 2
        pos = jnp.where(p > 2 * near, p, jnp.where(p % 2 == 1, near - step, near + step))
        return turned(pos)

    def place(zz, cc, hh, lo=0, size=feat):
        return T.at[aligned(zz * 2 + cc, rows), pl.ds(pl.multiple_of(hh * feat + lo, 128), size)]

    def uplace(zz, cc):
        return U.at[aligned(zz * 2 + cc, rows), :]

    def remote(src, dst, ss, rs, target):
        return pltpu.make_async_remote_copy(src_ref=src, dst_ref=dst, send_sem=ss, recv_sem=rs, device_id=target, device_id_type=MESH)

    my_up = up_ref.at[:, aligned(c, width)]
    their_up = up_ref.at[:, aligned(1 - c, width)]
    stays = [
        pltpu.make_async_copy(tok_ref, place(z, c, h), own.at[0]),
        pltpu.make_async_copy(my_up, uplace(z, c), own.at[1]),
        pltpu.make_async_copy(dec_ref, L.at[s], own.at[2]),
        pltpu.make_async_copy(seg_in, seg_ref, own.at[3]),
    ]

    def weight(hh):
        at = aligned(hh, feat)
        return [
            pltpu.make_async_copy(w_ref.at[at, aligned(c, width)], W.at[at, pl.ds(n * width, width)], wsem.at[hh, n])
            for n, w_ref in enumerate((wq_ref, wk_ref, wv_ref))
        ]

    everyone = [h] + others
    for copy in stays + weight(h):
        copy.start()

    def z_copy(src, zz, up):
        to = (z + 1 if up else z - 1) * 2 + c
        return remote(src, place(zz, c, h), zs.at[up, zz], zr.at[zz], (to, h))

    def ua_copy(src, zz, up):
        to = (z + 1 if up else z - 1) * 2 + c
        return remote(src, uplace(zz, c), uas.at[up, zz], uar.at[zz], (to, h))

    def ub_copy(zz, up):
        to = (z + 1 if up else z - 1) * 2 + c
        return remote(uplace(zz, 1 - c), uplace(zz, 1 - c), ubs.at[up, zz], ubr.at[zz], (to, h))

    def side_copy(src, zz, j, n):
        lo = n * piece
        return remote(src.at[:, pl.ds(lo, piece)], place(zz, c, h, lo, piece), xs.at[j, n, zz], xr.at[j, n, zz], (s, others[j]))

    def side_arrival(zz, j, n):
        here = place(zz, c, others[j], n * piece, piece)
        return remote(here, here, xs.at[j, n, zz], xr.at[j if relay else nh - 2 - j, n, zz], (mate, h))

    def diag_copy(zz, j):
        part = place(zz, c, others[j], j * piece, piece)
        return remote(part, part, ds.at[j, zz], dr.at[j, zz], (s, others[1 - j]))

    def diag_arrival(zz, j):
        part = place(zz, c, others[2], j * piece, piece)
        return remote(part, part, ds.at[j, zz], dr.at[j, zz], (mate, h))

    def mate_copy(zz, hh, n=0, size=feat):
        here = place(zz, c, hh, n * piece, size)
        return remote(here, here, ps.at[zz, hh, n], pr.at[zz, hh, n], (mate, h))

    def mate_arrival(zz, hh, n=0, size=feat):
        there = place(zz, 1 - c, hh, n * piece, size)
        return remote(there, there, ps.at[zz, hh, n], pr.at[zz, hh, n], (mate, h))

    def swap(b):
        return remote(A.at[0, aligned(b, rows)], A.at[1, aligned(b, rows)], es.at[b], er.at[b], (mate, h))

    mate_up = remote(their_up, uplace(z, c), qs.at[0], qr.at[0], (mate, h))

    def l_copy(zz, up):
        to = (z + 1 if up else z - 1) * 2 + c
        here = L.at[zz * 2 + c]
        return remote(here, here, ls.at[up, zz], lr.at[zz], (to, h))

    def l_mate(zz, cc):
        here = L.at[zz * 2 + cc]
        return remote(here, here, es2.at[zz], er2.at[zz], (mate, h))

    def spread(src, zz):
        for j in range(sides):
            side_copy(src, zz, j, j if relay else 0).start()
        if relay:
            for j in range(sides):
                side_copy(src, zz, j, 1 - j).start()
        mate_copy(zz, h).start()

    def along(zz, what):
        @pl.when((zz <= z) & goes_up)
        def _():
            what(1)

        @pl.when((zz >= z) & goes_down)
        def _():
            what(0)

    def each(k, what):
        for zz in (jnp.where(lower, z - k, z + k), jnp.where(lower, z + k, z - k)):
            pl.when((zz >= 0) & (zz < nz))(functools.partial(what, zz))

    def outer(zz):
        return (zz == 0) | (zz == nz - 1)

    def passed(zz):
        return ((zz < z) & goes_up) | ((zz > z) & goes_down)

    def take_z(k):
        def one(zz):
            here = place(zz, c, h)
            l_copy(zz, 0).wait_recv()
            l_mate(zz, c).start()
            along(zz, lambda up: l_copy(zz, up).start())
            z_copy(here, zz, 0).wait_recv()

            def forward(up):
                z_copy(here, zz, up).start()

                @pl.when(k == 1)
                def _():
                    ub_copy(z, up).start()

            along(zz, forward)
            pl.when(zz == order(k))(lambda: spread(here, zz))

        each(k, one)

    def wait_u(zz):
        ua_copy(uplace(zz, c), zz, 0).wait_recv()
        ub_copy(zz, 0).wait_recv()

    def pass_u(zz):
        @pl.when(passed(zz))
        def _():
            wait_u(zz)

            def forward(up):
                ua_copy(uplace(zz, c), zz, up).start()
                ub_copy(zz, up).start()

            along(zz, forward)

    for copy in stays:
        copy.wait()
    i = lax.broadcasted_iota(jnp.int32, (rows, rows), 0)
    j = lax.broadcasted_iota(jnp.int32, (rows, rows), 1)
    triangle = jnp.where(i <= j, 1.0, 0.0).astype(jnp.float32)
    L[s] = lax.dot_general(L[s], triangle, (((1,), (0,)), ((), ())), precision=lax.Precision.HIGHEST, preferred_element_type=jnp.float32)
    pl.semaphore_wait(barrier, 1 + len(others) + jnp.where(goes_up, 1, 0) + jnp.where(goes_down, 1, 0))
    mine = place(z, c, h)
    l_mate(z, c).start()
    along(z, lambda up: l_copy(z, up).start())
    along(z, lambda up: z_copy(mine, z, up).start())
    spread(mine, z)
    mate_up.start()
    along(z, lambda up: ua_copy(uplace(z, c), z, up).start())
    for hh in others:
        for copy in weight(hh):
            copy.start()

    def wide(row):
        return jnp.broadcast_to(row, (rows, rows))

    def start_up():
        there = uplace(z, 1 - c)
        remote(there, there, qs.at[0], qr.at[0], (mate, h)).wait_recv()

        @pl.when(goes_up & (z == 0))
        def _():
            ub_copy(z, 1).start()

        @pl.when(goes_down & (z == nz - 1))
        def _():
            ub_copy(z, 0).start()


    def pair(zz):
        return aligned(zz, 2 * rows)

    def project(p, hh, first=False, done=False, n=0, size=feat):
        zz, half_way = order(p), acc.at[p % 2]
        mate_arrival(zz, hh, n, size).wait_recv()
        some = pl.ds(pl.multiple_of(hh * feat + n * piece, size), size)
        for m, out in enumerate((q_s, k_s, v_s)):
            pick = slice(m * width, (m + 1) * width)
            new = dot(T[pair(zz), some], W[some, pick])
            if not first:
                new = half_way[:, pick] + new
            if done:
                out[pair(zz), :] = half(new)
            else:
                half_way[:, pick] = new

    def tables(zz):
        l_mate(zz, 1 - c).wait_recv()

        def block(b, _):
            segs = wide(seg_ref[pl.ds(b, 1), :].astype(jnp.float32))
            ahead = seg_ref[pl.ds(jnp.maximum(b - 1, 0), 1), rows - 1 :].astype(jnp.float32)
            before = wide(jnp.where(b == 0, -1.0, ahead))
            segs_down = segs.T
            last_seg = wide(segs[:1, rows - 1 :])
            same = (segs == segs_down) & (i >= j)
            for a in range(heads):
                ahead_sum = wide(L[b, pl.ds(c * heads + a, 1), :])
                down = ahead_sum.T
                last = wide(ahead_sum[:1, rows - 1 :])
                D[a, b] = jnp.where(same, SCALE * jnp.exp(jnp.where(same, down - ahead_sum, 0.0)), 0.0)
                IN[a, b] = jnp.where(segs_down == before, jnp.exp(down), 0.0)
                OUT[a, b] = jnp.where(segs_down == last_seg, jnp.exp(last - down), 0.0)
                CR[a, b + reach] = jnp.where(last_seg == before, jnp.exp(last), 0.0)[:8]
            return 0

        lax.fori_loop(zz * 2, zz * 2 + 2, block, 0)

    def prepare():
        zero = jnp.zeros((HEAD, HEAD), jnp.float32)
        for a in range(heads):
            for n in range(reach):
                for at in (n, nb + reach + n):
                    LT[a, at] = half(zero)
                    R[a, at] = half(zero)
                    CR[a, at] = zero[:8]

        def clear(n, _):
            G[:, aligned(n, 8), :] = jnp.zeros((2, 8, G.shape[2]), jnp.float32)
            return 0

        lax.fori_loop(0, G.shape[1] // 8, clear, 0)
        for copy in weight(h):
            copy.wait()
        project(0, h, first=True)
        tables(z)

    def cols(a):
        return slice(a * HEAD, (a + 1) * HEAD)

    def states(zz):
        for n in range(2):
            b = zz * 2 + n
            at = aligned(b, rows)
            for a in range(heads):
                weighted_k = half(OUT[a, b] * k_s[at, cols(a)].astype(jnp.float32))
                weighted_q = half(IN[a, b] * q_s[at, cols(a)].astype(jnp.float32))
                LT[a, b + reach] = half(dot(v_s[at, cols(a)], weighted_k, ((0,), (0,))))
                R[a, b + reach] = half(dot(weighted_q, U[at, cols(a)], ((0,), (0,))))

    def inside(zz):
        scores = []
        for n in range(2):
            b = zz * 2 + n
            at = aligned(b, rows)
            for a in range(heads):
                decay = D[a, b]
                attn_qk = half(decay * dot(q_s[at, cols(a)], k_s[at, cols(a)], ((1,), (1,))))
                attn_up = half(decay * dot(U[at, cols(a)], v_s[at, cols(a)], ((1,), (1,))))
                scores.append((n, a, attn_qk, attn_up))
        for n, a, attn_qk, attn_up in scores:
            at = aligned(zz * 2 + n, rows)
            put = aligned((zz % slots) * 2 + n, rows)
            B[put, cols(a)] = dot(attn_up, k_s[at, cols(a)])
            B[put, cols(heads + a)] = dot(attn_up, q_s[at, cols(a)], ((0,), (0,)))
            B[put, cols(2 * heads + a)] = dot(attn_qk, U[at, cols(a)], ((0,), (0,)))

    def between(zz):
        for n in range(2):
            b = zz * 2 + n
            at = aligned(b, rows)
            put = aligned((zz % slots) * 2 + n, rows)
            for a in range(heads):
                coming, back = whole(LT[a, b]), whole(R[a, b + 2 * reach])
                for m in range(reach - 1, 0, -1):
                    coming = wide(CR[a, b + reach - m, :1]) * coming + whole(LT[a, b + reach - m])
                    back = wide(CR[a, b + reach + m, :1]) * back + whole(R[a, b + reach + m])
                coming, back = half(SCALE * coming), half(SCALE * back)
                inflow, outflow = IN[a, b], OUT[a, b]
                in_u = half(inflow * U[at, cols(a)].astype(jnp.float32))
                out_v = half(outflow * v_s[at, cols(a)].astype(jnp.float32))
                out_k = half(outflow * k_s[at, cols(a)].astype(jnp.float32))
                terms = (dot(in_u, coming), dot(out_v, back, ((1,), (1,))), dot(out_k, back))
                for g, value in enumerate(terms):
                    A[0, at, cols(g * heads + a)] = half(B[put, cols(g * heads + a)] + value)
            swap(b).start()

    depth_rows = TT.shape[0]

    def turn(zz):
        TT[:, pair(zz)] = T[pair(zz), aligned(s, depth_rows)].T

    def gather(zz):
        swap(zz * 2).wait_recv()
        swap(zz * 2 + 1).wait_recv()
        for slot in range(2):
            for g in range(3):
                pick = slice(g * width, (g + 1) * width)
                G[slot, :, pick] += dot(TT[:, pair(zz)], A[slot, pair(zz), pick])

    prepare()

    def step(p, _):
        zz = order(p)
        live = p < nz

        @pl.when(live)
        def _():
            for n in range(sides):
                side_arrival(zz, n, n if relay else 0).wait_recv()
                if relay:
                    diag_copy(zz, n).start()
                    mate_copy(zz, others[n], n, piece).start()
                else:
                    mate_copy(zz, others[n]).start()

        pl.when(p == 0)(start_up)

        @pl.when(p == 2)
        def _():
            each(1, lambda zz: pl.when(jnp.logical_not(outer(zz)))(lambda: pass_u(zz)))

        @pl.when((p >= 1) & (p <= nz))
        def _():
            old = order(p - 1)

            @pl.when((old != z) & jnp.logical_not(passed(old)))
            def _():
                wait_u(old)

            states(old)
            turn(old)

        @pl.when((p >= 1) & live)
        def _():
            tables(zz)

        @pl.when(p + 1 < nz)
        def _():
            later = order(p + 1)
            pl.when(jnp.abs(later - z) <= p)(lambda: spread(place(later, c, h), later))
            take_z(p + 1)

        @pl.when(p == 1)
        def _():
            each(1, lambda zz: pl.when(outer(zz))(lambda: pass_u(zz)))

        @pl.when((p >= 2) & (p < nz))
        def _():
            each(p, pass_u)

        @pl.when((p >= 1) & (p <= nz))
        def _():
            inside(order(p - 1))

        @pl.when(p == 0)
        def _():
            for hh in others:
                for copy in weight(hh):
                    copy.wait()

        if relay:
            @pl.when(live)
            def _():
                for n in range(sides):
                    side_arrival(zz, n, 1 - n).wait_recv()
                    mate_copy(zz, others[n], 1 - n, piece).start()
                for n in range(sides):
                    project(p, others[n], n=n, size=piece)

        @pl.when(p >= lag + 1)
        def _():
            between(turned(p - lag - 1))

        @pl.when(p + 1 < nz)
        def _():
            project(p + 1, h, first=True)

        @pl.when(live)
        def _():
            if relay:
                def take_diag():
                    for n in range(2):
                        diag_arrival(zz, n).wait_recv()
                    mate_copy(zz, others[2]).start()

                pl.when(p + 1 < nz)(take_diag)
                for n in range(sides):
                    project(p, others[n], n=1 - n, size=piece)
                pl.when(p + 1 == nz)(take_diag)
            else:
                for n in range(sides):
                    project(p, others[n], done=n == sides - 1)

        @pl.when((p >= lag + 1) & live)
        def _():
            gather(turned(p - lag - 1))

        if relay:
            @pl.when(live)
            def _():
                project(p, others[2], done=True)

        return 0

    lax.fori_loop(0, nz + lag + 1, step, 0)
    late = lag + 1
    first = jnp.where(lower, nz - late, 0)
    final = turned(nz - 1)

    def run(start, count):
        return pl.ds(pl.multiple_of(start * 2 * rows, 2 * rows), count * 2 * rows)

    def finish(slot, at):
        put = aligned(c if slot == 0 else 1 - c, width)
        for g, out in enumerate((oq_ref, ok_ref, ov_ref)):
            pick = slice(g * width, (g + 1) * width)
            out[:, put] = half(G[slot, :, pick] + dot(TT[:, at], A[slot, at, pick]))

    finish(0, run(first, late))
    early = jnp.where(lower, nz - late, 1)
    for n in range(2 * late - 2):
        swap(early * 2 + n).wait_recv()
    for g in range(3):
        pick = slice(g * width, (g + 1) * width)
        G[1, :, pick] += dot(TT[:, run(early, late - 1)], A[1, run(early, late - 1), pick])
    for n in range(2):
        swap(final * 2 + n).wait_recv()
    finish(1, pair(final))

    def drain(zz, _):
        here = place(zz, c, h)

        def sent(up):
            z_copy(here, zz, up).wait_send()
            ua_copy(uplace(zz, c), zz, up).wait_send()
            ub_copy(zz, up).wait_send()
            l_copy(zz, up).wait_send()

        along(zz, sent)
        for n in range(sides):
            for m in range(parts):
                side_copy(here, zz, n, m).wait_send()
        if relay:
            for n in range(2):
                diag_copy(zz, n).wait_send()
        for n, hh in enumerate(everyone):
            if relay and 1 <= n <= 2:
                for m in range(2):
                    mate_copy(zz, hh, m, piece).wait_send()
            else:
                mate_copy(zz, hh).wait_send()
        swap(zz * 2).wait_send()
        swap(zz * 2 + 1).wait_send()
        l_mate(zz, c).wait_send()
        return 0

    lax.fori_loop(0, nz, drain, 0)
    mate_up.wait_send()


def store(a_ref, b_ref, c_ref, x_ref, y_ref, z_ref, sems):
    ends = ((a_ref, x_ref), (b_ref, y_ref), (c_ref, z_ref))
    copies = [pltpu.make_async_copy(src, dst, sems.at[n]) for n, (src, dst) in enumerate(ends)]
    for copy in copies:
        copy.start()
    for copy in copies:
        copy.wait()


def local(n_seq, nh, tokens, w_query, w_key, w_value, upstream, log_decay, segment):
    nz = n_seq // 2
    rows, feat = tokens.shape
    total, depth = rows * n_seq, feat * nh
    heads = w_query.shape[1] // HEAD // 2
    width = heads * HEAD
    reach = total // 4 // rows
    parts = 2 if nh == 4 else 1
    slots = 2 if nz <= 4 else nz
    decay = jnp.zeros((max(8, 2 * heads), rows), jnp.float32).at[: 2 * heads].set(log_decay.T)
    seg = segment.reshape(n_seq, rows)
    kind = tokens.dtype
    dma = pltpu.SemaphoreType.DMA
    vmem = pl.BlockSpec(memory_space=pltpu.VMEM)
    hbm = pl.BlockSpec(memory_space=pl.ANY)
    f32 = jnp.float32
    square = (HEAD, HEAD)
    padded = n_seq + 2 * reach
    out_rows = depth // n_seq
    grads = pl.pallas_call(
        functools.partial(kernel, nz, nh, heads, reach),
        out_shape=[pltpu.VMEM((out_rows, 2 * width), kind)] * 3,
        in_specs=[hbm] * 7,
        out_specs=[vmem] * 3,
        scratch_shapes=[
            pltpu.VMEM((total, depth), kind),
            pltpu.VMEM((total, width), kind),
            pltpu.VMEM((n_seq,) + decay.shape, f32),
            pltpu.VMEM(seg.shape, seg.dtype),
            pltpu.VMEM((depth, 3 * width), kind),
        ]
        + [pltpu.VMEM((total, width), kind)] * 3
        + [pltpu.VMEM((2, 2 * rows, 3 * width), f32)]
        + [pltpu.VMEM((heads, n_seq) + square, f32)] * 3
        + [pltpu.VMEM((heads, padded, 8, HEAD), f32)]
        + [pltpu.VMEM((heads, padded) + square, kind)] * 2
        + [
            pltpu.VMEM((2, total, 3 * width), kind),
            pltpu.VMEM((slots * 2 * rows, 3 * width), f32),
            pltpu.VMEM((out_rows, total), kind),
            pltpu.VMEM((2, out_rows, 3 * width), f32),
        ]
        + [dma((2, nz)), dma((nz,))] * 3
        + [dma((nh - 1, parts, nz))] * 2
        + [dma((2, nz))] * 2
        + [dma((nz, nh, parts))] * 2
        + [dma((1,))] * 2
        + [dma((n_seq,))] * 2
        + [dma((nz,))] * 2
        + [dma((2, nz)), dma((nz,))]
        + [dma((4,)), dma((nh, 3))],
        compiler_params=pltpu.CompilerParams(collective_id=0, has_side_effects=True, vmem_limit_bytes=VMEM_BYTES),
    )(tokens, upstream, decay, seg, w_query, w_key, w_value)
    return tuple(pl.pallas_call(
        store,
        out_shape=[jax.ShapeDtypeStruct((out_rows, 2 * width), kind)] * 3,
        in_specs=[vmem] * 3,
        out_specs=[hbm] * 3,
        scratch_shapes=[dma((3,))],
    )(*[pltpu.with_memory_space_constraint(grad, pltpu.VMEM) for grad in grads]))


def solution(mesh):
    placed = (P("seq", "head"), P(None, "head"), P(None, "head"), P(None, "head"), P("seq", "head"), P("seq", "head"), P())
    return jax.shard_map(
        functools.partial(local, mesh.shape["seq"], mesh.shape["head"]),
        mesh=mesh,
        in_specs=placed,
        out_specs=(P("seq", "head"),) * 3,
        check_vma=False,
    )
```
